32 devices in a mesh: row: 4 (over z), col: 4 (over x, core), depth: 2 (over y).
Axes of the slice: x: 2, y: 2, z: 4, core: 2. Of those that a mesh axis runs over, the one named last changes fastest.
Arguments:
- heads_concat: bfloat16 [2048, 16384], P('row', ('depth', 'col')), may hold values from -6 to 6
- w_out: bfloat16 [16384, 7168], P(('depth', 'row'), 'col'), may hold values from -0.046875 to 0.046875
Outputs:
- projected: bfloat16 [2048, 7168], P('row', ('col', 'depth'))
The draws below stay inside these ranges and needn't reach their ends.
All inputs are finite; a program needn't handle non-finite values.
Results may differ from the reference program's by a relative error of at most 0.001.
Values may be sent and summed in bfloat16 or wider, within the bound.
A program may use at most 128 MiB of HBM per device.

```python
import jax
import jax.numpy as jnp

D = 7168
K = 16384
TOKENS = 2048


def block_levels(stream_key, dims, cuts, least, top_value):
    factor_of, own = 1.0, jax.random.fold_in(stream_key, 6)
    for dim, parts in cuts:
        draws = jnp.exp(jax.random.uniform(jax.random.fold_in(own, dim), (parts,), jnp.float32, least / len(cuts), top_value / len(cuts)))
        factor_of = factor_of * jnp.repeat(draws, dims[dim] // parts).reshape([-1 if axis == dim else 1 for axis in range(len(dims))])
    return factor_of


def bell_draw(stream_key, extent, scale, limit, pieces=(), held_as=jnp.bfloat16):
    values = scale * jax.random.normal(stream_key, extent, jnp.float32)
    if pieces:
        values = values * block_levels(stream_key, extent, pieces, -0.22, 0.18)
    return jnp.clip(values, -limit, limit).astype(held_as)


def setup_inputs(seed: int = 0) -> dict:
    key_of = jax.random.split(jax.random.key(seed), 3)
    return {
        "heads_concat": bell_draw(key_of[0], (TOKENS, K), 1.0, 6.0, ((0, 4), (1, 8))),
        "w_out": bell_draw(key_of[1], (K, D), K ** -0.5, 0.046875, ((0, 8), (1, 4))),
    }


def reference(heads_concat, w_out):
    product = jnp.dot(heads_concat, w_out, preferred_element_type=jnp.float32)
    return product.astype(jnp.bfloat16)
```

```python
import functools

import jax
import jax.numpy as jnp
from jax import lax
from jax.experimental import pallas as pl
from jax.experimental.pallas import tpu as pltpu
from jax.sharding import PartitionSpec as P

MESH = pl.DeviceIdType.MESH
CORES = 2
LAG = 2
VMEM_BYTES = 66_000_000
SQUARINGS = 5
POWER = 2 ** SQUARINGS
REACH = 125
LOW = 2.0 ** (-REACH / POWER)
SPAN = 2.0 ** (REACH / POWER) - LOW
SMALLEST = 1e-36


def encode(value, coded, scale):
    largest = jnp.max(jnp.max(jnp.abs(value), axis=0, keepdims=True), axis=1, keepdims=True)
    largest = jnp.maximum(largest, SMALLEST)
    scale[...] = jnp.broadcast_to(largest, scale.shape)
    power = LOW + jnp.abs(value) * (SPAN / largest)
    for _ in range(SQUARINGS):
        power = power * power
    coded[...] = jnp.where(value < 0, -power, power).astype(coded.dtype)


def decode(coded, scale):
    power = coded[...].astype(jnp.float32)
    root = jnp.exp2(jnp.log2(jnp.abs(power)) * (1.0 / POWER))
    value = (root - LOW) * (scale[:, :1] * (1.0 / SPAN))
    return jnp.where(power < 0, -value, value)


def finishing(rows, r):
    downward = [(2 * t + rows - 1 - r, t) for t in range(r)]
    upward = [(2 * (rows - 1 - t) + r, t) for t in range(r + 1, rows)]
    return [t for _, t in sorted(downward + upward)] + [r]


def kernel(rows, cols, aligned, a_ref, w_ref, o_ref, w, a, own, out_y, in_y, out_z, chain,
           out_ys, in_ys, out_zs, chain_s,
           w_sem, s1_send, s1_recv, x_send, x_recv, c_send, c_recv, f_send, f_recv,
           y_send, y_recv, z_send, z_recv, ys_send, ys_recv, zs_send, zs_recv):
    r, j, d = lax.axis_index("row"), lax.axis_index("col"), lax.axis_index("depth")
    chips = cols // CORES
    x, core = j // CORES, j % CORES
    share = rows // cols
    tq, kb = a.shape[2], a.shape[3]
    nh = own.shape[3]
    steps = rows * cols
    mate = {"row": r, "col": x * CORES + 1 - core, "depth": d}
    across = {"row": r, "col": j, "depth": 1 - d}
    below = {"row": lax.rem(r + rows - 1, rows), "col": j, "depth": d}
    above = {"row": lax.rem(r + 1, rows), "col": j, "depth": d}
    source_col = r // share

    def x_col(dx):
        return lax.rem(x + dx, chips) * CORES + core

    def x_peer(dx):
        return {"row": r, "col": x_col(dx), "depth": d}

    w_copy = pltpu.make_async_copy(w_ref, w, w_sem)
    w_copy.start()

    barrier = pltpu.get_barrier_semaphore()

    def greet(device):
        pl.semaphore_signal(barrier, inc=1, device_id=device, device_id_type=MESH)

    for t in range(rows):
        pl.when(jnp.logical_or(r != t, source_col != j))(
            lambda t=t: greet({"row": t, "col": source_col, "depth": d})
        )
    for dx in range(1, chips):
        greet(x_peer(dx))
    greet(mate)
    greet(across)
    pl.when(r > 0)(lambda: greet(below))
    pl.when(r < rows - 1)(lambda: greet(above))
    pl.semaphore_wait(
        barrier,
        share * cols + chips
        + jnp.where(source_col != j, 1, 0)
        + jnp.where(r > 0, 1, 0)
        + jnp.where(r < rows - 1, 1, 0),
    )

    def remote(src, dst, send, recv, device):
        return pltpu.make_async_remote_copy(
            src_ref=src, dst_ref=dst, send_sem=send, recv_sem=recv,
            device_id=device, device_id_type=MESH,
        )

    def first(i, q):
        target = {"row": j * share + i, "col": q, "depth": d}
        source = a_ref.at[pl.ds(q * tq, tq), pl.ds(i * kb, kb)]
        return remote(source, a.at[r, q], s1_send.at[i, q], s1_recv.at[r], target)

    def is_me(i, q):
        return jnp.logical_and(r == j * share + i, j == q)

    for i in range(share):
        for q in range(cols):
            @pl.when(is_me(i, q))
            def _():
                pltpu.make_async_copy(
                    a_ref.at[pl.ds(q * tq, tq), pl.ds(i * kb, kb)],
                    a.at[r, q], s1_recv.at[r],
                ).start()

            @pl.when(jnp.logical_not(is_me(i, q)))
            def _():
                first(i, q).start()

    def to_x(t, dx):
        return remote(a.at[t, j], a.at[t, j], x_send.at[dx - 1, t], x_recv.at[dx - 1, t], x_peer(dx))

    def to_mate(t):
        return remote(a.at[t, j], a.at[t, j], c_send.at[t], c_recv.at[t], mate)

    def forward(t, dx):
        col = x_col(chips - dx)
        return remote(a.at[t, col], a.at[t, col], f_send.at[dx - 1, t], f_recv.at[dx - 1, t], mate)

    def arrived(slot, sem):
        pltpu.make_async_copy(slot, slot, sem).wait()

    def spread(t):
        arrived(a.at[t, j], s1_recv.at[t])
        for dx in range(1, chips):
            to_x(t, dx).start()
        to_mate(t).start()

    def relay(t):
        for dx in range(1, chips):
            arrived(a.at[t, x_col(chips - dx)], x_recv.at[dx - 1, t])
            forward(t, dx).start()

    def half(h):
        if aligned:
            return w[:, pl.ds(pl.multiple_of(h * nh, 128), nh)]
        return w[h]

    def y_copies(t, q):
        return (
            remote(out_y.at[t, q], in_y.at[t, q], y_send.at[t, q], y_recv.at[t, q], across),
            remote(out_ys.at[t, q], in_ys.at[t, q], ys_send.at[t, q], ys_recv.at[t, q], across),
        )

    def z_copies(t, q, slot, device):
        return (
            remote(out_z.at[t, q], chain.at[slot, q], z_send.at[t, q], z_recv.at[slot, q], device),
            remote(out_zs.at[t, q], chain_s.at[slot, q], zs_send.at[t, q], zs_recv.at[slot, q], device),
        )

    def down(t, q):
        return z_copies(t, q, t, below)

    def up(t, q):
        return z_copies(t, q, t + 1, above)

    def start(copies):
        for copy in copies:
            copy.start()

    def wait_send(copies):
        for copy in copies:
            copy.wait_send()

    order = []
    for p in range(rows):
        block = jnp.int32(0)
        for row in range(rows):
            block = jnp.where(r == row, finishing(rows, row)[p], block)
        order.append(block)

    def pick(p):
        block = order[0]
        for n in range(1, rows):
            block = jnp.where(p == n, order[n], block)
        return block

    def place(n):
        k = n // (CORES * (rows - 1)) * CORES + n % CORES
        return n // CORES % (rows - 1), k

    def column(k):
        chip = lax.rem(x + chips - k // CORES, chips)
        return chip * CORES + jnp.where(k % CORES == 0, core, 1 - core)

    def multiply(t, q):
        block = a[t, q]
        sent = jnp.dot(block, half(1 - d), preferred_element_type=jnp.float32)
        encode(sent, out_y.at[t, q], out_ys.at[t, q])
        start(y_copies(t, q))
        own[t, q] = jnp.dot(block, half(d), preferred_element_type=jnp.float32)

    def finish(s):
        p, k = place(s)
        mine = s >= steps - cols
        t = jnp.where(mine, r, pick(p))
        q = column(jnp.where(mine, s - (steps - cols), k))
        arrived(in_y.at[t, q], y_recv.at[t, q])
        arrived(in_ys.at[t, q], ys_recv.at[t, q])
        own[t, q] += decode(in_y.at[t, q], in_ys.at[t, q])

        def add(slot):
            arrived(chain.at[slot, q], z_recv.at[slot, q])
            arrived(chain_s.at[slot, q], zs_recv.at[slot, q])
            own[t, q] += decode(chain.at[slot, q], chain_s.at[slot, q])

        pl.when(jnp.logical_and(t <= r, r < rows - 1))(lambda: add(t))
        pl.when(jnp.logical_and(t >= r, r > 0))(lambda: add(t + 1))
        pl.when(t != r)(lambda: encode(own[t, q], out_z.at[t, q], out_zs.at[t, q]))
        pl.when(t < r)(lambda: start(down(t, q)))
        pl.when(t > r)(lambda: start(up(t, q)))

        @pl.when(t == r)
        def _():
            o_ref[pl.ds(pl.multiple_of(q * tq, tq), tq), :] = own[t, q].astype(o_ref.dtype)

    w_copy.wait()

    def step(s, carry):
        p, k = place(s - cols)
        mine = s < cols
        t = jnp.where(mine, r, pick(p))
        k = jnp.where(mine, s, k)

        pl.when(k == 0)(lambda: spread(t))

        @pl.when(k == 1)
        def _():
            arrived(a.at[t, column(1)], c_recv.at[t])

        pl.when(k == CORES)(lambda: relay(t))
        for dx in range(1, chips):
            @pl.when(k == CORES * dx + 1)
            def _():
                arrived(a.at[t, column(CORES * dx + 1)], f_recv.at[dx - 1, t])

        multiply(t, column(k))

        pl.when(s >= cols + LAG)(lambda: finish(s - cols - LAG))
        return carry

    lax.fori_loop(0, steps, step, 0)

    def last(s, carry):
        finish(s)
        return carry

    lax.fori_loop(steps - cols - LAG, steps, last, 0)

    for i in range(share):
        for q in range(cols):
            pl.when(jnp.logical_not(is_me(i, q)))(lambda i=i, q=q: first(i, q).wait_send())

    def drain(t, carry):
        for dx in range(1, chips):
            to_x(t, dx).wait_send()
            forward(t, dx).wait_send()
        to_mate(t).wait_send()
        for q in range(cols):
            wait_send(y_copies(t, q))
            pl.when(t != r)(lambda q=q: wait_send(down(t, q)))
        return carry

    lax.fori_loop(0, rows, drain, 0)


def project(rows, cols, heads, w_out):
    tokens = heads.shape[0]
    kb, n = w_out.shape
    nh, tq = n // 2, tokens // cols
    chips = cols // CORES
    aligned = nh % 128 == 0
    w_shape = (kb, n)
    if not aligned:
        w_out = jnp.stack([w_out[:, :nh], w_out[:, nh:]])
        w_shape = (2, kb, nh)
    dma = pltpu.SemaphoreType.DMA
    f32 = jnp.float32
    return pl.pallas_call(
        functools.partial(kernel, rows, cols, aligned),
        out_shape=jax.ShapeDtypeStruct((tokens, nh), jnp.bfloat16),
        in_specs=[pl.BlockSpec(memory_space=pltpu.HBM)] * 2,
        out_specs=pl.BlockSpec(memory_space=pltpu.VMEM),
        scratch_shapes=[
            pltpu.VMEM(w_shape, jnp.bfloat16),
            pltpu.VMEM((rows, cols, tq, kb), jnp.bfloat16),
            pltpu.VMEM((rows, cols, tq, nh), f32),
            pltpu.VMEM((rows, cols, tq, nh), jnp.bfloat16),
            pltpu.VMEM((rows, cols, tq, nh), jnp.bfloat16),
            pltpu.VMEM((rows, cols, tq, nh), jnp.bfloat16),
            pltpu.VMEM((rows + 1, cols, tq, nh), jnp.bfloat16),
            pltpu.VMEM((rows, cols, 1, 128), f32),
            pltpu.VMEM((rows, cols, 1, 128), f32),
            pltpu.VMEM((rows, cols, 1, 128), f32),
            pltpu.VMEM((rows + 1, cols, 1, 128), f32),
            dma,
            dma((rows // cols, cols)), dma((rows,)),
            dma((chips - 1, rows)), dma((chips - 1, rows)),
            dma((rows,)), dma((rows,)),
            dma((chips - 1, rows)), dma((chips - 1, rows)),
            dma((rows, cols)), dma((rows, cols)),
            dma((rows, cols)), dma((rows + 1, cols)),
            dma((rows, cols)), dma((rows, cols)),
            dma((rows, cols)), dma((rows + 1, cols)),
        ],
        compiler_params=pltpu.CompilerParams(
            collective_id=0, has_side_effects=True, vmem_limit_bytes=VMEM_BYTES
        ),
    )(heads, w_out)


def solution(mesh):
    rows, cols = mesh.shape["row"], mesh.shape["col"]

    def per_device(heads, w_out):
        tokens, n = heads.shape[0], w_out.shape[1]
        lanes = -(-n // 256) * 128
        slots = 17 * rows * tokens * lanes
        calls = 1
        while slots // calls > VMEM_BYTES // 2:
            calls *= 2
        size = tokens // calls
        parts = [
            project(rows, cols, heads[c * size:(c + 1) * size], w_out)
            for c in range(calls)
        ]
        return parts[0] if calls == 1 else jnp.concatenate(parts, axis=0)

    return jax.shard_map(
        per_device,
        mesh=mesh,
        in_specs=(P("row", ("depth", "col")), P(("depth", "row"), "col")),
        out_specs=P("row", ("col", "depth")),
        check_vma=False,
    )
```

```python
import functools

import jax
import jax.numpy as jnp
from jax import lax
from jax.experimental import pallas as pl
from jax.experimental.pallas import tpu as pltpu
from jax.sharding import PartitionSpec as P

MESH = pl.DeviceIdType.MESH
CORES = 2
LAGS = (6, 1, 2)
CALM_STEP = (2, 0)
PASS_STEPS = ((0, 0), (1, 0))
FEED_STEP = 1
PASS_CALM = (1, 1)
SPREAD_NEAR = (1, -1)
SPREAD_FAR = (0, 0)
RELAY_NEAR = (4, 6)
RELAY_FAR = (2, 2)
ADJOINING_X = (5, 7)
VMEM_BYTES = 66_000_000
SQUARINGS = 5
POWER = 2 ** SQUARINGS
REACH = 125
LOW = 2.0 ** (-REACH / POWER)
SPAN = 2.0 ** (REACH / POWER) - LOW
SMALLEST = 1e-36


def encode(value, coded, scale):
    largest = jnp.max(jnp.max(jnp.abs(value), axis=0, keepdims=True), axis=1, keepdims=True)
    largest = jnp.maximum(largest, SMALLEST)
    scale[...] = jnp.broadcast_to(largest, scale.shape)
    power = LOW + jnp.abs(value) * (SPAN / largest)
    for _ in range(SQUARINGS):
        power = power * power
    coded[...] = jnp.where(value < 0, -power, power).astype(coded.dtype)


def decode(coded, scale):
    power = coded[...].astype(jnp.float32)
    root = jnp.exp2(jnp.log2(jnp.abs(power)) * (1.0 / POWER))
    value = (root - LOW) * (scale[:, :1] * (1.0 / SPAN))
    return jnp.where(power < 0, -value, value)


def adjoining(row):
    return row + 1 - 2 * (row % 2)


def finishing(rows, r, near, paired):
    downward = [(2 * t + rows - 1 - r, t) for t in range(r)]
    upward = [(2 * (rows - 1 - t) + r, t) for t in range(r + 1, rows)]
    everyone = [t for _, t in sorted(downward + upward)]
    if not paired:
        return everyone
    others = [t for t in everyone if t != adjoining(r)]
    return [adjoining(r)] + others if near else others + [adjoining(r)]


def pairable(rows, cols):
    for x in range(cols // CORES):
        place = {}
        for r in range(rows):
            near = r * cols // rows // CORES == x
            for p, t in enumerate(finishing(rows, r, near, True)):
                place[r, t] = p
        for r, t in place:
            before = (r + 1, t) if t < r else (r - 1, t)
            if place.get(before, 0) > place[r, t]:
                return False
    return True


def kernel(rows, cols, aligned, a_ref, w_ref, o_ref, w, a, via, own, out_y, in_y, out_z, chain,
           out_ys, in_ys, out_zs, chain_s,
           w_sem, own_x_send, own_m_send, own_recv, adj_send, adj_x_send, adj_recv, adj_m_send, adj_m_recv,
           v_send, v_recv, s1_send, s1_recv,
           x_send, x_recv, c_send, c_recv, f_send, f_recv,
           y_send, y_recv, z_send, z_recv, ys_send, ys_recv, zs_send, zs_recv):
    r, j, d = lax.axis_index("row"), lax.axis_index("col"), lax.axis_index("depth")
    chips = cols // CORES
    x, core = j // CORES, j % CORES
    share = rows // cols
    tq, kb = a.shape[2], a.shape[3]
    nh = own.shape[3]
    steps = rows * cols
    mate = {"row": r, "col": x * CORES + 1 - core, "depth": d}
    across = {"row": r, "col": j, "depth": 1 - d}
    below = {"row": lax.rem(r + rows - 1, rows), "col": j, "depth": d}
    above = {"row": lax.rem(r + 1, rows), "col": j, "depth": d}
    source_col = r // share
    source_x, source_core = source_col // CORES, source_col % CORES
    home = j == source_col
    paired = pairable(rows, cols)
    near = jnp.logical_and(x == source_x, paired)
    edge = jnp.logical_or(r == 0, r == rows - 1)
    beside = adjoining(r) if paired else -1

    def x_at(dx):
        return lax.rem(x + dx, chips)

    def x_col(dx):
        return x_at(dx) * CORES + core

    def x_peer(dx):
        return {"row": r, "col": x_col(dx), "depth": d}

    w_copy = pltpu.make_async_copy(w_ref, w, w_sem)
    w_copy.start()

    barrier = pltpu.get_barrier_semaphore()

    def greet(device):
        pl.semaphore_signal(barrier, inc=1, device_id=device, device_id_type=MESH)

    for t in range(rows):
        pl.when(r != t)(
            lambda t=t: greet({"row": t, "col": x * CORES + source_core, "depth": d})
        )
    for dx in range(1, chips):
        greet(x_peer(dx))
    greet(mate)
    greet(across)
    pl.when(r > 0)(lambda: greet(below))
    pl.when(r < rows - 1)(lambda: greet(above))
    pl.semaphore_wait(
        barrier,
        CORES * (rows // CORES - jnp.where(source_core == core, 1, 0)) + chips + 1
        + jnp.where(r > 0, 1, 0)
        + jnp.where(r < rows - 1, 1, 0),
    )

    def remote(src, dst, send, recv, device):
        return pltpu.make_async_remote_copy(
            src_ref=src, dst_ref=dst, send_sem=send, recv_sem=recv,
            device_id=device, device_id_type=MESH,
        )

    def arrived(slot, sem):
        pltpu.make_async_copy(slot, slot, sem).wait()

    def piece(i, q):
        return a_ref.at[pl.ds(pl.multiple_of(q * tq, tq), tq), pl.ds(pl.multiple_of(i * kb, kb), kb)]

    def target(dx, i):
        return x_col(chips - dx) * share + i

    def away(dx, i):
        return jnp.logical_and(target(dx, i) != r, target(dx, i) != beside)

    def urgent(dx, i):
        return r == jnp.where(target(dx, i) < rows // 2, rows - 1, 0)

    def send(dx, i, c):
        col = x * CORES + c
        source = via.at[dx - 1, i, c] if dx else piece(i, col)
        device = {"row": target(dx, i), "col": col, "depth": d}
        return remote(source, a.at[r, col], s1_send.at[dx, i, c], s1_recv.at[r], device)

    def aside(dx, i, c):
        return remote(
            piece(i, x_at(dx) * CORES + c), via.at[dx - 1, i, c],
            v_send.at[dx - 1, i, c], v_recv.at[dx - 1, i, c], x_peer(dx),
        )

    def own_x(dx, q):
        return remote(piece(r % share, q), a.at[r, q], own_x_send.at[dx - 1, q], own_recv.at[q], x_peer(dx))

    def own_mate(q, source):
        return remote(source, a.at[r, q], own_m_send.at[q], own_recv.at[q], mate)

    def early(dx, i):
        return jnp.logical_or(urgent(dx, i), x_at(chips - dx) != source_x)

    def column(k):
        chip = lax.rem(x + chips - k // CORES, chips)
        return chip * CORES + jnp.where(k % CORES == 0, core, 1 - core)

    def adjoin(e, c):
        col = lax.rem(x + chips - e, chips) * CORES + c
        device = {"row": beside, "col": x * CORES + c, "depth": d}
        return remote(piece(beside % share, col), a.at[r, col], adj_send.at[e, c], adj_recv.at[e], device)

    def adjoin_x(e, dx):
        slot = a.at[beside, column(CORES * e)]
        index = lax.rem(e + dx, chips)
        return remote(slot, slot, adj_x_send.at[dx - 1, e], adj_recv.at[index], x_peer(dx))

    def adjoin_mate(e):
        slot = a.at[beside, column(CORES * e)]
        return remote(slot, slot, adj_m_send.at[e], adj_m_recv.at[e], mate)

    feeds = jnp.logical_and(beside // share == j, paired)

    def feed(es):
        @pl.when(feeds)
        def _():
            for e in es:
                for c in range(CORES):
                    adjoin(e, c).start()

    feed([0])

    for i in range(share):
        for c in range(CORES):
            pl.when(jnp.logical_and(away(0, i), urgent(0, i)))(lambda i=i, c=c: send(0, i, c).start())
            for dx in range(1, chips):
                pl.when(away(0, i))(lambda dx=dx, i=i, c=c: aside(dx, i, c).start())

    @pl.when(home)
    def _():
        for q in range(cols):
            pltpu.make_async_copy(piece(r % share, q), a.at[r, q], own_recv.at[q]).start()
            own_mate(q, piece(r % share, q)).start()
            for dx in range(1, chips):
                own_x(dx, q).start()

    carrier = jnp.logical_and(core == source_core, x != source_x)

    def own_ready(q):
        arrived(a.at[r, q], own_recv.at[q])
        pl.when(carrier)(lambda: own_mate(q, a.at[r, q]).start())

    def calm(dx, i):
        return jnp.logical_not(urgent(dx, i))

    def each(dxs, cs, chosen, act):
        for i in range(share):
            for c in cs:
                for dx in dxs:
                    pl.when(jnp.logical_and(away(dx, i), chosen(dx, i)))(
                        lambda dx=dx, i=i, c=c: act(dx, i, c)
                    )

    def pass_on(dx, i, c):
        arrived(via.at[dx - 1, i, c], v_recv.at[dx - 1, i, c])
        send(dx, i, c).start()

    def adjoining_ready(k):
        e = k // CORES

        @pl.when(k % CORES == 0)
        def _():
            arrived(a.at[beside, column(k)], adj_recv.at[e])
            adjoin_mate(e).start()

        @pl.when(k % CORES == 1)
        def _():
            arrived(a.at[beside, column(k)], adj_m_recv.at[e])

    def to_x(t, dx):
        return remote(a.at[t, j], a.at[t, j], x_send.at[dx - 1, t], x_recv.at[dx - 1, t], x_peer(dx))

    def to_mate(t):
        return remote(a.at[t, j], a.at[t, j], c_send.at[t], c_recv.at[t], mate)

    def forward(t, dx):
        col = x_col(chips - dx)
        return remote(a.at[t, col], a.at[t, col], f_send.at[dx - 1, t], f_recv.at[dx - 1, t], mate)

    def spread(t):
        arrived(a.at[t, j], s1_recv.at[t])
        for dx in range(1, chips):
            to_x(t, dx).start()
        to_mate(t).start()

    def relay(t):
        for dx in range(1, chips):
            arrived(a.at[t, x_col(chips - dx)], x_recv.at[dx - 1, t])
            forward(t, dx).start()

    def half(h):
        if aligned:
            return w[:, pl.ds(pl.multiple_of(h * nh, 128), nh)]
        return w[h]

    def y_copies(t, q):
        return (
            remote(out_y.at[t, q], in_y.at[t, q], y_send.at[t, q], y_recv.at[t, q], across),
            remote(out_ys.at[t, q], in_ys.at[t, q], ys_send.at[t, q], ys_recv.at[t, q], across),
        )

    def z_copies(t, q, slot, device):
        return (
            remote(out_z.at[t, q], chain.at[slot, q], z_send.at[t, q], z_recv.at[slot, q], device),
            remote(out_zs.at[t, q], chain_s.at[slot, q], zs_send.at[t, q], zs_recv.at[slot, q], device),
        )

    def down(t, q):
        return z_copies(t, q, t, below)

    def up(t, q):
        return z_copies(t, q, t + 1, above)

    def start(copies):
        for copy in copies:
            copy.start()

    def wait_send(copies):
        for copy in copies:
            copy.wait_send()

    order = []
    for p in range(rows - 1):
        block = jnp.int32(0)
        for row in range(rows):
            close, distant = finishing(rows, row, True, paired)[p], finishing(rows, row, False, paired)[p]
            block = jnp.where(r == row, jnp.where(near, close, distant), block)
        order.append(block)

    def pick(p):
        block = order[0]
        for n in range(1, rows - 1):
            block = jnp.where(p == n, order[n], block)
        return block

    def tile(n):
        block, k = n // cols, n % cols
        if not paired:
            return pick(block), k
        first = n < CORES
        inner = jnp.logical_and(n >= CORES, n < CORES + cols)
        outer = jnp.logical_and(n >= CORES + cols, n < 2 * cols)
        near_t = jnp.where(inner, pick(1), jnp.where(jnp.logical_or(first, outer), beside, pick(block)))
        near_k = jnp.where(inner, n - CORES, jnp.where(outer, n - cols, k))
        far_t = pick(block)
        far_k = jnp.where(far_t == beside, (k + CORES) % cols, k)
        return jnp.where(near, near_t, far_t), jnp.where(near, near_k, far_k)

    def multiply(t, q):
        block = a[t, q]
        sent = jnp.dot(block, half(1 - d), preferred_element_type=jnp.float32)
        encode(sent, out_y.at[t, q], out_ys.at[t, q])
        start(y_copies(t, q))
        own[t, q] = jnp.dot(block, half(d), preferred_element_type=jnp.float32)

    def finish(s):
        mine = s >= steps - cols
        t, k = tile(jnp.where(mine, 0, s))
        t = jnp.where(mine, r, t)
        q = jnp.where(mine, s % cols, column(k))
        arrived(in_y.at[t, q], y_recv.at[t, q])
        arrived(in_ys.at[t, q], ys_recv.at[t, q])
        own[t, q] += decode(in_y.at[t, q], in_ys.at[t, q])

        def add(slot):
            arrived(chain.at[slot, q], z_recv.at[slot, q])
            arrived(chain_s.at[slot, q], zs_recv.at[slot, q])
            own[t, q] += decode(chain.at[slot, q], chain_s.at[slot, q])

        pl.when(jnp.logical_and(t <= r, r < rows - 1))(lambda: add(t))
        pl.when(jnp.logical_and(t >= r, r > 0))(lambda: add(t + 1))
        pl.when(t != r)(lambda: encode(own[t, q], out_z.at[t, q], out_zs.at[t, q]))
        pl.when(t < r)(lambda: start(down(t, q)))
        pl.when(t > r)(lambda: start(up(t, q)))

        @pl.when(t == r)
        def _():
            o_ref[pl.ds(pl.multiple_of(q * tq, tq), tq), :] = own[t, q].astype(o_ref.dtype)

    w_copy.wait()

    lag = jnp.where(near, jnp.where(edge, LAGS[2], LAGS[0]), LAGS[1])

    def at(s, near_step, far_step):
        return s == jnp.where(near, near_step, far_step)

    def split(p):
        return jnp.where(near, pick(min(p + 1, rows - 2)), pick(p))

    def step(s, carry):
        mine = s < cols
        t, k = tile(jnp.where(mine, 0, s - cols))
        t = jnp.where(mine, r, t)
        k = jnp.where(mine, s, k)
        q = jnp.where(mine, k, column(k))
        adjoined = jnp.logical_and(jnp.logical_not(mine), t == beside)
        divided = jnp.logical_and(jnp.logical_not(mine), t != beside)
        peers = range(1, chips)

        for c in range(CORES):
            pl.when(at(s, cols + PASS_STEPS[c][0], cols + PASS_STEPS[c][1]))(
                lambda c=c: each(peers, [c], urgent, pass_on)
            )
        pl.when(at(s, cols + FEED_STEP, cols))(lambda: feed(range(1, chips)))
        pl.when(at(s, cols + CALM_STEP[0], cols + CALM_STEP[1]))(
            lambda: each([0], range(CORES), calm, lambda dx, i, c: send(dx, i, c).start())
        )
        pl.when(at(s, cols + PASS_CALM[0], cols + PASS_CALM[1]))(
            lambda: each(peers, range(CORES), calm, pass_on)
        )
        for p in range(rows - 2 if paired else rows - 1):
            base = cols * (p + 1)

            @pl.when(at(s, base + SPREAD_NEAR[min(p, 1)], base + SPREAD_FAR[min(p, 1)]))
            def _():
                spread(split(p))

            @pl.when(at(s, base + RELAY_NEAR[min(p, 1)], base + RELAY_FAR[min(p, 1)]))
            def _():
                relay(split(p))

        for e in range(chips):
            @pl.when(jnp.logical_and(near, s == cols + ADJOINING_X[min(e, 1)]))
            def _():
                for dx in peers:
                    adjoin_x(e, dx).start()

        pl.when(mine)(lambda: own_ready(k))
        pl.when(adjoined)(lambda: adjoining_ready(k))

        @pl.when(jnp.logical_and(divided, k == 1))
        def _():
            arrived(a.at[t, column(1)], c_recv.at[t])

        for dx in peers:
            @pl.when(jnp.logical_and(divided, k == CORES * dx + 1))
            def _():
                arrived(a.at[t, column(CORES * dx + 1)], f_recv.at[dx - 1, t])

        multiply(t, q)

        pl.when(s >= cols + lag)(lambda: finish(s - cols - lag))
        return carry

    lax.fori_loop(0, steps, step, 0)

    def last(s, carry):
        finish(s)
        return carry

    lax.fori_loop(steps - cols - lag, steps, last, 0)

    for e in range(chips):
        for c in range(CORES):
            pl.when(feeds)(lambda e=e, c=c: adjoin(e, c).wait_send())
        pl.when(paired)(lambda e=e: adjoin_mate(e).wait_send())
        for dx in range(1, chips):
            pl.when(near)(lambda e=e, dx=dx: adjoin_x(e, dx).wait_send())

    for i in range(share):
        for c in range(CORES):
            for dx in range(chips):
                pl.when(away(dx, i))(lambda dx=dx, i=i, c=c: send(dx, i, c).wait_send())
                if dx:
                    pl.when(away(0, i))(lambda dx=dx, i=i, c=c: aside(dx, i, c).wait_send())

    for q in range(cols):
        @pl.when(core == source_core)
        def _():
            own_mate(q, a.at[r, q]).wait_send()

        @pl.when(home)
        def _():
            for dx in range(1, chips):
                own_x(dx, q).wait_send()

    def drain(t, carry):
        @pl.when(jnp.logical_and(t != r, t != beside))
        def _():
            for dx in range(1, chips):
                to_x(t, dx).wait_send()
                forward(t, dx).wait_send()
            to_mate(t).wait_send()
        for q in range(cols):
            wait_send(y_copies(t, q))
            pl.when(t != r)(lambda q=q: wait_send(down(t, q)))
        return carry

    lax.fori_loop(0, rows, drain, 0)


def project(rows, cols, heads, w_out):
    tokens = heads.shape[0]
    kb, n = w_out.shape
    nh, tq = n // 2, tokens // cols
    chips, share = cols // CORES, rows // cols
    aligned = nh % 128 == 0
    w_shape = (kb, n)
    if not aligned:
        w_out = jnp.stack([w_out[:, :nh], w_out[:, nh:]])
        w_shape = (2, kb, nh)
    dma = pltpu.SemaphoreType.DMA
    f32 = jnp.float32
    return pl.pallas_call(
        functools.partial(kernel, rows, cols, aligned),
        out_shape=jax.ShapeDtypeStruct((tokens, nh), jnp.bfloat16),
        in_specs=[pl.BlockSpec(memory_space=pltpu.HBM)] * 2,
        out_specs=pl.BlockSpec(memory_space=pltpu.VMEM),
        scratch_shapes=[
            pltpu.VMEM(w_shape, jnp.bfloat16),
            pltpu.VMEM((rows, cols, tq, kb), jnp.bfloat16),
            pltpu.VMEM((chips - 1, share, CORES, tq, kb), jnp.bfloat16),
            pltpu.VMEM((rows, cols, tq, nh), f32),
            pltpu.VMEM((rows, cols, tq, nh), jnp.bfloat16),
            pltpu.VMEM((rows, cols, tq, nh), jnp.bfloat16),
            pltpu.VMEM((rows, cols, tq, nh), jnp.bfloat16),
            pltpu.VMEM((rows + 1, cols, tq, nh), jnp.bfloat16),
            pltpu.VMEM((rows, cols, 1, 128), f32),
            pltpu.VMEM((rows, cols, 1, 128), f32),
            pltpu.VMEM((rows, cols, 1, 128), f32),
            pltpu.VMEM((rows + 1, cols, 1, 128), f32),
            dma,
            dma((chips - 1, cols)), dma((cols,)), dma((cols,)),
            dma((chips, CORES)), dma((chips - 1, chips)), dma((chips,)), dma((chips,)), dma((chips,)),
            dma((chips - 1, share, CORES)), dma((chips - 1, share, CORES)),
            dma((chips, share, CORES)), dma((rows,)),
            dma((chips - 1, rows)), dma((chips - 1, rows)),
            dma((rows,)), dma((rows,)),
            dma((chips - 1, rows)), dma((chips - 1, rows)),
            dma((rows, cols)), dma((rows, cols)),
            dma((rows, cols)), dma((rows + 1, cols)),
            dma((rows, cols)), dma((rows, cols)),
            dma((rows, cols)), dma((rows + 1, cols)),
        ],
        compiler_params=pltpu.CompilerParams(
            collective_id=0, has_side_effects=True, vmem_limit_bytes=VMEM_BYTES
        ),
    )(heads, w_out)


def solution(mesh):
    rows, cols = mesh.shape["row"], mesh.shape["col"]

    def per_device(heads, w_out):
        tokens, n = heads.shape[0], w_out.shape[1]
        lanes = -(-n // 256) * 128
        slots = 17 * rows * tokens * lanes
        calls = 1
        while slots // calls > VMEM_BYTES // 2:
            calls *= 2
        size = tokens // calls
        parts = [
            project(rows, cols, heads[c * size:(c + 1) * size], w_out)
            for c in range(calls)
        ]
        return parts[0] if calls == 1 else jnp.concatenate(parts, axis=0)

    return jax.shard_map(
        per_device,
        mesh=mesh,
        in_specs=(P("row", ("depth", "col")), P(("depth", "row"), "col")),
        out_specs=P("row", ("col", "depth")),
        check_vma=False,
    )
```

```python
import functools

import jax
import jax.numpy as jnp
from jax import lax
from jax.experimental import pallas as pl
from jax.experimental.pallas import tpu as pltpu
from jax.sharding import PartitionSpec as P

MESH = pl.DeviceIdType.MESH
CORES = 2
LAGS = (5, 1, 1)
GRAIN = 2
CALM_STEP = (2, -3)
PASS_STEPS = ((0, 0), (1, 0))
FEED_STEP = 1
PASS_CALM = (1, 1)
SPREAD_NEAR = (1, 0)
SPREAD_FAR = (0, 0)
RELAY_NEAR = (4, 6)
RELAY_FAR = (2, 2)
ADJOINING_X = (5, 7)
VMEM_BYTES = 66_000_000
SQUARINGS = 5
POWER = 2 ** SQUARINGS
REACH = 125
LOW = 2.0 ** (-REACH / POWER)
SPAN = 2.0 ** (REACH / POWER) - LOW
SMALLEST = 1e-36


def encode(value, coded, scale):
    largest = jnp.max(jnp.max(jnp.abs(value), axis=0, keepdims=True), axis=1, keepdims=True)
    largest = jnp.maximum(largest, SMALLEST)
    scale[...] = jnp.broadcast_to(largest, scale.shape)
    power = LOW + jnp.abs(value) * (SPAN / largest)
    for _ in range(SQUARINGS):
        power = power * power
    coded[...] = jnp.where(value < 0, -power, power).astype(coded.dtype)


def decode(coded, scale):
    power = coded[...].astype(jnp.float32)
    root = jnp.exp2(jnp.log2(jnp.abs(power)) * (1.0 / POWER))
    value = (root - LOW) * (scale[:, :1] * (1.0 / SPAN))
    return jnp.where(power < 0, -value, value)


def adjoining(row):
    return row + 1 - 2 * (row % 2)


def finishing(rows, r, near, paired):
    downward = [(2 * t + rows - 1 - r, t) for t in range(r)]
    upward = [(2 * (rows - 1 - t) + r, t) for t in range(r + 1, rows)]
    everyone = [t for _, t in sorted(downward + upward)]
    if not paired:
        return everyone
    others = [t for t in everyone if t != adjoining(r)]
    return [adjoining(r)] + others if near else others + [adjoining(r)]


def pairable(rows, cols):
    for x in range(cols // CORES):
        place = {}
        for r in range(rows):
            near = r * cols // rows // CORES == x
            for p, t in enumerate(finishing(rows, r, near, True)):
                place[r, t] = p
        for r, t in place:
            before = (r + 1, t) if t < r else (r - 1, t)
            if place.get(before, 0) > place[r, t]:
                return False
    return True


def kernel(rows, cols, aligned, a_ref, w_ref, o_ref, w, a, via, own, out_y, in_y, out_z, chain,
           out_ys, in_ys, out_zs, chain_s,
           w_sem, own_x_send, own_m_send, own_recv, adj_send, adj_x_send, adj_recv, adj_m_send, adj_m_recv,
           v_send, v_recv, s1_send, s1_recv,
           x_send, x_recv, c_send, c_recv, f_send, f_recv,
           y_send, y_recv, z_send, z_recv, ys_send, ys_recv, zs_send, zs_recv):
    r, j, d = lax.axis_index("row"), lax.axis_index("col"), lax.axis_index("depth")
    chips = cols // CORES
    x, core = j // CORES, j % CORES
    share = rows // cols
    tq, kb = a.shape[2], a.shape[3]
    nh = own.shape[3]
    steps = rows * cols
    mate = {"row": r, "col": x * CORES + 1 - core, "depth": d}
    across = {"row": r, "col": j, "depth": 1 - d}
    below = {"row": lax.rem(r + rows - 1, rows), "col": j, "depth": d}
    above = {"row": lax.rem(r + 1, rows), "col": j, "depth": d}
    source_col = r // share
    source_x, source_core = source_col // CORES, source_col % CORES
    home = j == source_col
    paired = pairable(rows, cols)
    near = jnp.logical_and(x == source_x, paired)
    edge = jnp.logical_or(r == 0, r == rows - 1)
    beside = adjoining(r) if paired else -1

    def x_at(dx):
        return lax.rem(x + dx, chips)

    def x_col(dx):
        return x_at(dx) * CORES + core

    def x_peer(dx):
        return {"row": r, "col": x_col(dx), "depth": d}

    w_copy = pltpu.make_async_copy(w_ref, w, w_sem)
    w_copy.start()

    barrier = pltpu.get_barrier_semaphore()

    def greet(device):
        pl.semaphore_signal(barrier, inc=1, device_id=device, device_id_type=MESH)

    for t in range(rows):
        pl.when(r != t)(
            lambda t=t: greet({"row": t, "col": x * CORES + source_core, "depth": d})
        )
    for dx in range(1, chips):
        greet(x_peer(dx))
    greet(mate)
    greet(across)
    pl.when(r > 0)(lambda: greet(below))
    pl.when(r < rows - 1)(lambda: greet(above))
    pl.semaphore_wait(
        barrier,
        CORES * (rows // CORES - jnp.where(source_core == core, 1, 0)) + chips + 1
        + jnp.where(r > 0, 1, 0)
        + jnp.where(r < rows - 1, 1, 0),
    )

    def remote(src, dst, send, recv, device):
        return pltpu.make_async_remote_copy(
            src_ref=src, dst_ref=dst, send_sem=send, recv_sem=recv,
            device_id=device, device_id_type=MESH,
        )

    def arrived(slot, sem):
        pltpu.make_async_copy(slot, slot, sem).wait()

    grain = s1_recv.shape[1]
    ts = tq // grain

    def piece(i, q):
        return a_ref.at[pl.ds(pl.multiple_of(q * tq, tq), tq), pl.ds(pl.multiple_of(i * kb, kb), kb)]

    def part(i, q, g):
        return a_ref.at[
            pl.ds(pl.multiple_of(q * tq + g * ts, ts), ts), pl.ds(pl.multiple_of(i * kb, kb), kb)
        ]

    def sub(g):
        return pl.ds(g * ts, ts)

    def target(dx, i):
        return x_col(chips - dx) * share + i

    def away(dx, i):
        return jnp.logical_and(target(dx, i) != r, target(dx, i) != beside)

    def urgent(dx, i):
        return r == jnp.where(target(dx, i) < rows // 2, rows - 1, 0)

    def send(dx, i, c, g):
        col = x * CORES + c
        source = via.at[dx - 1, i, c, sub(g)] if dx else part(i, col, g)
        device = {"row": target(dx, i), "col": col, "depth": d}
        return remote(source, a.at[r, col, sub(g)], s1_send.at[dx, i, c, g], s1_recv.at[r, g], device)

    def aside(dx, i, c, g):
        return remote(
            part(i, x_at(dx) * CORES + c, g), via.at[dx - 1, i, c, sub(g)],
            v_send.at[dx - 1, i, c, g], v_recv.at[dx - 1, i, c, g], x_peer(dx),
        )

    def start_send(dx, i, c):
        for g in range(grain):
            send(dx, i, c, g).start()

    def start_aside(dx, i, c):
        for g in range(grain):
            aside(dx, i, c, g).start()

    def own_x(dx, q):
        return remote(piece(r % share, q), a.at[r, q], own_x_send.at[dx - 1, q], own_recv.at[q], x_peer(dx))

    def own_mate(q, source):
        return remote(source, a.at[r, q], own_m_send.at[q], own_recv.at[q], mate)

    def early(dx, i):
        return jnp.logical_or(urgent(dx, i), x_at(chips - dx) != source_x)

    def column(k):
        chip = lax.rem(x + chips - k // CORES, chips)
        return chip * CORES + jnp.where(k % CORES == 0, core, 1 - core)

    def adjoin(e, c):
        col = lax.rem(x + chips - e, chips) * CORES + c
        device = {"row": beside, "col": x * CORES + c, "depth": d}
        return remote(piece(beside % share, col), a.at[r, col], adj_send.at[e, c], adj_recv.at[e], device)

    def adjoin_x(e, dx):
        slot = a.at[beside, column(CORES * e)]
        index = lax.rem(e + dx, chips)
        return remote(slot, slot, adj_x_send.at[dx - 1, e], adj_recv.at[index], x_peer(dx))

    def adjoin_mate(e):
        slot = a.at[beside, column(CORES * e)]
        return remote(slot, slot, adj_m_send.at[e], adj_m_recv.at[e], mate)

    feeds = jnp.logical_and(beside // share == j, paired)

    def feed(es):
        @pl.when(feeds)
        def _():
            for e in es:
                for c in range(CORES):
                    adjoin(e, c).start()

    feed([0])

    for i in range(share):
        for c in range(CORES):
            pl.when(jnp.logical_and(away(0, i), urgent(0, i)))(lambda i=i, c=c: start_send(0, i, c))
            for dx in range(1, chips):
                pl.when(away(0, i))(lambda dx=dx, i=i, c=c: start_aside(dx, i, c))

    @pl.when(home)
    def _():
        for q in range(cols):
            pltpu.make_async_copy(piece(r % share, q), a.at[r, q], own_recv.at[q]).start()
            own_mate(q, piece(r % share, q)).start()
            for dx in range(1, chips):
                own_x(dx, q).start()

    carrier = jnp.logical_and(core == source_core, x != source_x)

    def own_ready(q):
        arrived(a.at[r, q], own_recv.at[q])
        pl.when(carrier)(lambda: own_mate(q, a.at[r, q]).start())

    def calm(dx, i):
        return jnp.logical_not(urgent(dx, i))

    def each(dxs, cs, chosen, act):
        for i in range(share):
            for c in cs:
                for dx in dxs:
                    pl.when(jnp.logical_and(away(dx, i), chosen(dx, i)))(
                        lambda dx=dx, i=i, c=c: act(dx, i, c)
                    )

    def pass_on(dx, i, c):
        for g in range(grain):
            arrived(via.at[dx - 1, i, c, sub(g)], v_recv.at[dx - 1, i, c, g])
            send(dx, i, c, g).start()

    def adjoining_ready(k):
        e = k // CORES

        @pl.when(k % CORES == 0)
        def _():
            arrived(a.at[beside, column(k)], adj_recv.at[e])
            adjoin_mate(e).start()

        @pl.when(k % CORES == 1)
        def _():
            arrived(a.at[beside, column(k)], adj_m_recv.at[e])

    def to_x(t, dx, g):
        slot = a.at[t, j, sub(g)]
        return remote(slot, slot, x_send.at[dx - 1, t, g], x_recv.at[dx - 1, t], x_peer(dx))

    def to_mate(t):
        return remote(a.at[t, j], a.at[t, j], c_send.at[t], c_recv.at[t], mate)

    def forward(t, dx):
        col = x_col(chips - dx)
        return remote(a.at[t, col], a.at[t, col], f_send.at[dx - 1, t], f_recv.at[dx - 1, t], mate)

    def spread(t):
        for g in range(grain):
            arrived(a.at[t, j, sub(g)], s1_recv.at[t, g])
            for dx in range(1, chips):
                to_x(t, dx, g).start()
        to_mate(t).start()

    def relay(t):
        for dx in range(1, chips):
            arrived(a.at[t, x_col(chips - dx)], x_recv.at[dx - 1, t])
            forward(t, dx).start()

    def half(h):
        if aligned:
            return w[:, pl.ds(pl.multiple_of(h * nh, 128), nh)]
        return w[h]

    def y_copies(t, q):
        return (
            remote(out_y.at[t, q], in_y.at[t, q], y_send.at[t, q], y_recv.at[t, q], across),
            remote(out_ys.at[t, q], in_ys.at[t, q], ys_send.at[t, q], ys_recv.at[t, q], across),
        )

    def z_copies(t, q, slot, device):
        return (
            remote(out_z.at[t, q], chain.at[slot, q], z_send.at[t, q], z_recv.at[slot, q], device),
            remote(out_zs.at[t, q], chain_s.at[slot, q], zs_send.at[t, q], zs_recv.at[slot, q], device),
        )

    def down(t, q):
        return z_copies(t, q, t, below)

    def up(t, q):
        return z_copies(t, q, t + 1, above)

    def start(copies):
        for copy in copies:
            copy.start()

    def wait_send(copies):
        for copy in copies:
            copy.wait_send()

    order = []
    for p in range(rows - 1):
        block = jnp.int32(0)
        for row in range(rows):
            close, distant = finishing(rows, row, True, paired)[p], finishing(rows, row, False, paired)[p]
            block = jnp.where(r == row, jnp.where(near, close, distant), block)
        order.append(block)

    def pick(p):
        block = order[0]
        for n in range(1, rows - 1):
            block = jnp.where(p == n, order[n], block)
        return block

    def tile(n):
        block, k = n // cols, n % cols
        if not paired:
            return pick(block), k
        first = n < CORES
        inner = jnp.logical_and(n >= CORES, n < CORES + cols)
        outer = jnp.logical_and(n >= CORES + cols, n < 2 * cols)
        near_t = jnp.where(inner, pick(1), jnp.where(jnp.logical_or(first, outer), beside, pick(block)))
        near_k = jnp.where(inner, n - CORES, jnp.where(outer, n - cols, k))
        far_t = pick(block)
        far_k = jnp.where(far_t == beside, (k + CORES) % cols, k)
        return jnp.where(near, near_t, far_t), jnp.where(near, near_k, far_k)

    def multiply(t, q):
        block = a[t, q]
        sent = jnp.dot(block, half(1 - d), preferred_element_type=jnp.float32)
        encode(sent, out_y.at[t, q], out_ys.at[t, q])
        start(y_copies(t, q))
        own[t, q] = jnp.dot(block, half(d), preferred_element_type=jnp.float32)

    def finish(s):
        mine = s >= steps - cols
        t, k = tile(jnp.where(mine, 0, s))
        t = jnp.where(mine, r, t)
        q = jnp.where(mine, s % cols, column(k))
        arrived(in_y.at[t, q], y_recv.at[t, q])
        arrived(in_ys.at[t, q], ys_recv.at[t, q])
        own[t, q] += decode(in_y.at[t, q], in_ys.at[t, q])

        def add(slot):
            arrived(chain.at[slot, q], z_recv.at[slot, q])
            arrived(chain_s.at[slot, q], zs_recv.at[slot, q])
            own[t, q] += decode(chain.at[slot, q], chain_s.at[slot, q])

        pl.when(jnp.logical_and(t <= r, r < rows - 1))(lambda: add(t))
        pl.when(jnp.logical_and(t >= r, r > 0))(lambda: add(t + 1))
        pl.when(t != r)(lambda: encode(own[t, q], out_z.at[t, q], out_zs.at[t, q]))
        pl.when(t < r)(lambda: start(down(t, q)))
        pl.when(t > r)(lambda: start(up(t, q)))

        @pl.when(t == r)
        def _():
            o_ref[pl.ds(pl.multiple_of(q * tq, tq), tq), :] = own[t, q].astype(o_ref.dtype)

    w_copy.wait()

    lag = jnp.where(near, jnp.where(edge, LAGS[2], LAGS[0]), LAGS[1])

    def at(s, near_step, far_step):
        return s == jnp.where(near, near_step, far_step)

    def split(p):
        return jnp.where(near, pick(min(p + 1, rows - 2)), pick(p))

    def step(s, carry):
        mine = s < cols
        t, k = tile(jnp.where(mine, 0, s - cols))
        t = jnp.where(mine, r, t)
        k = jnp.where(mine, s, k)
        q = jnp.where(mine, k, column(k))
        adjoined = jnp.logical_and(jnp.logical_not(mine), t == beside)
        divided = jnp.logical_and(jnp.logical_not(mine), t != beside)
        peers = range(1, chips)

        for c in range(CORES):
            pl.when(at(s, cols + PASS_STEPS[c][0], cols + PASS_STEPS[c][1]))(
                lambda c=c: each(peers, [c], urgent, pass_on)
            )
        pl.when(at(s, cols + FEED_STEP, cols))(lambda: feed(range(1, chips)))
        pl.when(at(s, cols + CALM_STEP[0], cols + CALM_STEP[1]))(
            lambda: each([0], range(CORES), calm, start_send)
        )
        pl.when(at(s, cols + PASS_CALM[0], cols + PASS_CALM[1]))(
            lambda: each(peers, range(CORES), calm, pass_on)
        )
        for p in range(rows - 2 if paired else rows - 1):
            base = cols * (p + 1)

            @pl.when(at(s, base + SPREAD_NEAR[min(p, 1)], base + SPREAD_FAR[min(p, 1)]))
            def _():
                spread(split(p))

            @pl.when(at(s, base + RELAY_NEAR[min(p, 1)], base + RELAY_FAR[min(p, 1)]))
            def _():
                relay(split(p))

        for e in range(chips):
            @pl.when(jnp.logical_and(near, s == cols + ADJOINING_X[min(e, 1)]))
            def _():
                for dx in peers:
                    adjoin_x(e, dx).start()

        pl.when(mine)(lambda: own_ready(k))
        pl.when(adjoined)(lambda: adjoining_ready(k))

        @pl.when(jnp.logical_and(divided, k == 1))
        def _():
            arrived(a.at[t, column(1)], c_recv.at[t])

        for dx in peers:
            @pl.when(jnp.logical_and(divided, k == CORES * dx + 1))
            def _():
                arrived(a.at[t, column(CORES * dx + 1)], f_recv.at[dx - 1, t])

        multiply(t, q)

        pl.when(s >= cols + lag)(lambda: finish(s - cols - lag))
        return carry

    lax.fori_loop(0, steps, step, 0)

    def last(s, carry):
        finish(s)
        return carry

    lax.fori_loop(steps - cols - lag, steps, last, 0)

    for e in range(chips):
        for c in range(CORES):
            pl.when(feeds)(lambda e=e, c=c: adjoin(e, c).wait_send())
        pl.when(paired)(lambda e=e: adjoin_mate(e).wait_send())
        for dx in range(1, chips):
            pl.when(near)(lambda e=e, dx=dx: adjoin_x(e, dx).wait_send())

    for i in range(share):
        for c in range(CORES):
            for dx in range(chips):
                for g in range(grain):
                    pl.when(away(dx, i))(lambda dx=dx, i=i, c=c, g=g: send(dx, i, c, g).wait_send())
                    if dx:
                        pl.when(away(0, i))(lambda dx=dx, i=i, c=c, g=g: aside(dx, i, c, g).wait_send())

    for q in range(cols):
        @pl.when(core == source_core)
        def _():
            own_mate(q, a.at[r, q]).wait_send()

        @pl.when(home)
        def _():
            for dx in range(1, chips):
                own_x(dx, q).wait_send()

    def drain(t, carry):
        @pl.when(jnp.logical_and(t != r, t != beside))
        def _():
            for dx in range(1, chips):
                for g in range(grain):
                    to_x(t, dx, g).wait_send()
                forward(t, dx).wait_send()
            to_mate(t).wait_send()
        for q in range(cols):
            wait_send(y_copies(t, q))
            pl.when(t != r)(lambda q=q: wait_send(down(t, q)))
        return carry

    lax.fori_loop(0, rows, drain, 0)


def project(rows, cols, heads, w_out):
    tokens = heads.shape[0]
    kb, n = w_out.shape
    nh, tq = n // 2, tokens // cols
    chips, share = cols // CORES, rows // cols
    grain = GRAIN if tq % (16 * GRAIN) == 0 else 1
    aligned = nh % 128 == 0
    w_shape = (kb, n)
    if not aligned:
        w_out = jnp.stack([w_out[:, :nh], w_out[:, nh:]])
        w_shape = (2, kb, nh)
    dma = pltpu.SemaphoreType.DMA
    f32 = jnp.float32
    return pl.pallas_call(
        functools.partial(kernel, rows, cols, aligned),
        out_shape=jax.ShapeDtypeStruct((tokens, nh), jnp.bfloat16),
        in_specs=[pl.BlockSpec(memory_space=pltpu.HBM)] * 2,
        out_specs=pl.BlockSpec(memory_space=pltpu.VMEM),
        scratch_shapes=[
            pltpu.VMEM(w_shape, jnp.bfloat16),
            pltpu.VMEM((rows, cols, tq, kb), jnp.bfloat16),
            pltpu.VMEM((chips - 1, share, CORES, tq, kb), jnp.bfloat16),
            pltpu.VMEM((rows, cols, tq, nh), f32),
            pltpu.VMEM((rows, cols, tq, nh), jnp.bfloat16),
            pltpu.VMEM((rows, cols, tq, nh), jnp.bfloat16),
            pltpu.VMEM((rows, cols, tq, nh), jnp.bfloat16),
            pltpu.VMEM((rows + 1, cols, tq, nh), jnp.bfloat16),
            pltpu.VMEM((rows, cols, 1, 128), f32),
            pltpu.VMEM((rows, cols, 1, 128), f32),
            pltpu.VMEM((rows, cols, 1, 128), f32),
            pltpu.VMEM((rows + 1, cols, 1, 128), f32),
            dma,
            dma((chips - 1, cols)), dma((cols,)), dma((cols,)),
            dma((chips, CORES)), dma((chips - 1, chips)), dma((chips,)), dma((chips,)), dma((chips,)),
            dma((chips - 1, share, CORES, grain)), dma((chips - 1, share, CORES, grain)),
            dma((chips, share, CORES, grain)), dma((rows, grain)),
            dma((chips - 1, rows, grain)), dma((chips - 1, rows)),
            dma((rows,)), dma((rows,)),
            dma((chips - 1, rows)), dma((chips - 1, rows)),
            dma((rows, cols)), dma((rows, cols)),
            dma((rows, cols)), dma((rows + 1, cols)),
            dma((rows, cols)), dma((rows, cols)),
            dma((rows, cols)), dma((rows + 1, cols)),
        ],
        compiler_params=pltpu.CompilerParams(
            collective_id=0, has_side_effects=True, vmem_limit_bytes=VMEM_BYTES
        ),
    )(heads, w_out)


def solution(mesh):
    rows, cols = mesh.shape["row"], mesh.shape["col"]

    def per_device(heads, w_out):
        tokens, n = heads.shape[0], w_out.shape[1]
        lanes = -(-n // 256) * 128
        slots = 17 * rows * tokens * lanes
        calls = 1
        while slots // calls > VMEM_BYTES // 2:
            calls *= 2
        size = tokens // calls
        parts = [
            project(rows, cols, heads[c * size:(c + 1) * size], w_out)
            for c in range(calls)
        ]
        return parts[0] if calls == 1 else jnp.concatenate(parts, axis=0)

    return jax.shard_map(
        per_device,
        mesh=mesh,
        in_specs=(P("row", ("depth", "col")), P(("depth", "row"), "col")),
        out_specs=P("row", ("col", "depth")),
        check_vma=False,
    )
```
